32 devices in a mesh: seq: 8 (over z, core), tp: 4 (over y, x).
Axes of the slice: x: 2, y: 2, z: 4, core: 2. Of those that a mesh axis runs over, the one named last changes fastest.
Arguments:
- tokens: bfloat16 [1024, 8192], P('seq'), may hold values from -6 to 6
- conv_weight: float32 [4, 8192], replicated, may hold values from -3 to 3
- norm_gain: float32 [8192], replicated, may hold values from 0.25 to 1.75
- gate_weight: bfloat16 [8192, 14336], P('seq', 'tp'), may hold values from -0.0625 to 0.0625
- up_weight: bfloat16 [8192, 14336], P('seq', 'tp'), may hold values from -0.0625 to 0.0625
- down_weight: bfloat16 [14336, 8192], P('tp', 'seq'), may hold values from -0.046875 to 0.046875
Outputs:
- mixed_out: bfloat16 [1024, 8192], P(('seq', 'tp'))
The draws below stay inside these ranges and needn't reach their ends.
All inputs are finite; a program needn't handle non-finite values.
Results may differ from the reference program's by a relative error of at most 0.03.
Values may be sent and summed in bfloat16 or wider, within the bound.
A program may use at most 128 MiB of HBM per device.

```python
import jax
import jax.numpy as jnp
from jax import lax

D = 8192
FF = 14336
TAPS = 4
TOKENS = 1024
N_SEQ = 8


def levels(key, dims, cuts, low, largest):
    def one(axis_at, parts):
        steps = jax.random.uniform(jax.random.fold_in(jax.random.fold_in(key, 6), axis_at), (parts,), jnp.float32, low / len(cuts), largest / len(cuts))
        return jnp.repeat(jnp.exp(steps), dims[axis_at] // parts).reshape((-1,) + (1,) * (len(dims) - axis_at - 1))

    loudness = one(*cuts[0])
    for cut in cuts[1:]:
        loudness = loudness * one(*cut)
    return loudness


def scatter_about(key, dims, deviation, limit, split=(), dtype=jnp.bfloat16):
    array = deviation * jax.random.normal(key, dims, jnp.float32)
    if split:
        array = array * levels(key, dims, split, -0.22, 0.18)
    return jnp.clip(array, -limit, limit).astype(dtype)


def setup_inputs(seed: int = 0) -> dict:
    keys = jax.random.split(jax.random.key(seed), 7)
    return {
        "tokens": scatter_about(keys[0], (TOKENS, D), 1.0, 6.0, ((0, 8),)),
        "conv_weight": scatter_about(keys[1], (TAPS, D), 0.5, 3.0, (), jnp.float32),
        "norm_gain": jnp.clip(1.0 + 0.15 * jax.random.normal(keys[2], (D,), jnp.float32), 0.25, 1.75),
        "gate_weight": scatter_about(keys[3], (D, FF), D ** -0.5, 0.0625, ((0, 8), (1, 4))),
        "up_weight": scatter_about(keys[4], (D, FF), D ** -0.5, 0.0625, ((0, 8), (1, 4))),
        "down_weight": scatter_about(keys[5], (FF, D), FF ** -0.5, 0.046875, ((0, 4), (1, 8))),
    }


def reference(tokens, conv_weight, norm_gain, gate_weight, up_weight, down_weight):
    inputs = tokens.astype(jnp.float32)
    tok_count = inputs.shape[0]
    model_width = inputs.shape[1]
    taps_count = conv_weight.shape[0]
    padded = jnp.concatenate([jnp.zeros((taps_count - 1, model_width), jnp.float32), inputs], 0)
    conv_out = jnp.zeros((tok_count, model_width), jnp.float32)
    for tap_index in range(taps_count):
        begin = taps_count - 1 - tap_index
        conv_out = conv_out + conv_weight[tap_index][None, :] * padded[begin:begin + tok_count]
    scale_rms = lax.rsqrt(lax.optimization_barrier(jnp.mean(conv_out * conv_out, axis=-1, keepdims=True)) + 1e-05)
    normed = (conv_out * scale_rms * norm_gain[None, :]).astype(jnp.bfloat16)
    group_width = model_width // N_SEQ
    hidden_width = gate_weight.shape[1]
    gate = jnp.zeros((tok_count, hidden_width), jnp.float32)
    up_sum = jnp.zeros((tok_count, hidden_width), jnp.float32)
    for group_index in range(N_SEQ):
        lower = group_index * group_width
        feats = normed[:, lower:lower + group_width]
        gate_part = jnp.dot(feats, gate_weight[lower:lower + group_width], preferred_element_type=jnp.float32)
        up_part = jnp.dot(feats, up_weight[lower:lower + group_width], preferred_element_type=jnp.float32)
        gate = gate + lax.optimization_barrier(gate_part.astype(jnp.bfloat16)).astype(jnp.float32)
        up_sum = up_sum + lax.optimization_barrier(up_part.astype(jnp.bfloat16)).astype(jnp.float32)
    hidden = (jax.nn.silu(gate) * up_sum).astype(jnp.bfloat16)
    return jnp.dot(hidden, down_weight, preferred_element_type=jnp.float32).astype(jnp.bfloat16)
```

```python
import functools

import jax
import jax.numpy as jnp
from jax import lax
from jax.experimental import pallas as pl
from jax.experimental.pallas import tpu as pltpu
from jax.sharding import PartitionSpec as P

MESH = pl.DeviceIdType.MESH
WIDTH = 256
BLOCK_TOKENS = 1024
RS_LAG = 1
AG_LAG = 1


def from_behind(shard, axis, by):
    peers = lax.axis_size(axis)
    pairs = [(i, i + by) for i in range(peers) if 0 <= i + by < peers]
    return lax.ppermute(shard, axis, pairs)


def ffn_kernel(seq_n, tp_n, x_ref, gw_ref, uw_ref, dw_ref, out_ref, x_all, w_buf, d_buf, own, give, got, chain, hid, acc,
               x_snd, x_rcv, x_loc, w_sem, d_sem, p_snd, p_rcv, c_snd, c_rcv, h_snd, h_rcv, q_snd, q_rcv):
    stops = seq_n // 2
    seq_i = lax.axis_index("seq")
    tp_i = lax.axis_index("tp")
    pos = seq_i // 2
    core = seq_i % 2
    partner = (pos * 2 + 1 - core, tp_i)

    def at_stop(stop):
        return (stop * 2 + core, tp_i)

    sub = x_ref.shape[0]
    tokens = sub * tp_n
    half = tokens // 2
    quarter = half // 2
    chunks = gw_ref.shape[1] // WIDTH

    def w_copies(c):
        slot = c % 2
        cols = pl.ds(pl.multiple_of(c * WIDTH, WIDTH), WIDTH)
        return [
            pltpu.make_async_copy(gw_ref.at[:, cols], w_buf.at[slot, 0], w_sem.at[slot, 0]),
            pltpu.make_async_copy(uw_ref.at[:, cols], w_buf.at[slot, 1], w_sem.at[slot, 1]),
        ]

    for c in range(2):
        for cp in w_copies(c):
            cp.start()
    d_copy = pltpu.make_async_copy(dw_ref, d_buf, d_sem)
    d_copy.start()
    my_x = pl.ds(pl.multiple_of(tp_i * sub, sub), sub)
    x_own = pltpu.make_async_copy(x_ref, x_all.at[my_x], x_loc)
    x_own.start()

    barrier = pltpu.get_barrier_semaphore()
    greet = [partner, at_stop((pos + 1) % stops), at_stop((pos + stops - 1) % stops)]
    greet += [(seq_i, (tp_i + j) % tp_n) for j in range(1, tp_n)]
    for dev in greet:
        pl.semaphore_signal(barrier, inc=1, device_id=dev, device_id_type=MESH)
    pl.semaphore_wait(barrier, len(greet))

    def x_copy(j):
        return pltpu.make_async_remote_copy(
            src_ref=x_ref, dst_ref=x_all.at[my_x], send_sem=x_snd.at[j], recv_sem=x_rcv.at[j],
            device_id=(seq_i, (tp_i + j + 1) % tp_n), device_id_type=MESH)

    def x_land(j):
        origin = (tp_i + tp_n - j - 1) % tp_n
        rows = pl.ds(pl.multiple_of(origin * sub, sub), sub)
        return pltpu.make_async_remote_copy(
            src_ref=x_ref, dst_ref=x_all.at[rows], send_sem=x_snd.at[j], recv_sem=x_rcv.at[j],
            device_id=(seq_i, (tp_i + j + 1) % tp_n), device_id_type=MESH)

    for j in range(tp_n - 1):
        x_copy(j).start()
    acc[...] = jnp.zeros_like(acc)
    x_own.wait()
    for j in range(tp_n - 1):
        x_land(j).wait_recv()

    def swap_copy(c, h):
        return pltpu.make_async_remote_copy(
            src_ref=give.at[c, h], dst_ref=got.at[c, h], send_sem=p_snd.at[h, c], recv_sem=p_rcv.at[h, c],
            device_id=partner, device_id_type=MESH)

    def step_of(h):
        return -1 if h == 0 else 1

    def clamp(stop):
        return jnp.clip(stop, 0, stops - 1)

    def chain_copy(c, h):
        return pltpu.make_async_remote_copy(
            src_ref=got.at[c, h], dst_ref=chain.at[c, h], send_sem=c_snd.at[h, c], recv_sem=c_rcv.at[h, c],
            device_id=at_stop(pos + step_of(h)), device_id_type=MESH)

    def back_copy(c, h):
        return pltpu.make_async_remote_copy(
            src_ref=hid.at[c, h, core], dst_ref=hid.at[c, h, core], send_sem=h_snd.at[h, c], recv_sem=h_rcv.at[h, c],
            device_id=at_stop(pos - step_of(h)), device_id_type=MESH)

    def side_copy(c, h):
        return pltpu.make_async_remote_copy(
            src_ref=hid.at[c, h, core], dst_ref=hid.at[c, h, core], send_sem=q_snd.at[h, c], recv_sem=q_rcv.at[h, c],
            device_id=partner, device_id_type=MESH)

    def side_land(c, h):
        return pltpu.make_async_remote_copy(
            src_ref=hid.at[c, h, 1 - core], dst_ref=hid.at[c, h, 1 - core], send_sem=q_snd.at[h, c],
            recv_sem=q_rcv.at[h, c], device_id=partner, device_id_type=MESH)

    def done_before(h):
        return stops - 1 - pos if h == 0 else pos

    def inside(c):
        return jnp.logical_and(c >= 0, c < chunks)

    def multiply(c):
        slot = c % 2
        for cp in w_copies(c):
            cp.wait()
        for h in range(2):
            for mine in range(2):
                q = core if mine else 1 - core
                rows = x_all[pl.ds(pl.multiple_of(h * half + q * quarter, quarter), quarter), :]
                dest = own if mine else give
                for k in range(2):
                    part = jnp.dot(rows, w_buf[slot, k], preferred_element_type=jnp.float32)
                    dest[c, h, :, k * WIDTH : (k + 1) * WIDTH] = part.astype(jnp.bfloat16)
        for h in range(2):
            swap_copy(c, h).start()

        @pl.when(c + 2 < chunks)
        def _():
            for cp in w_copies(c + 2):
                cp.start()

    def reduce(c, h):
        swap_copy(c, h).wait_recv()
        before = done_before(h)
        total = lambda: own[c, h].astype(jnp.float32) + got[c, h].astype(jnp.float32)

        @pl.when(before == 0)
        def _():
            got[c, h] = total().astype(jnp.bfloat16)

        @pl.when(before > 0)
        def _():
            chain_copy(c, h).wait_recv()

        @pl.when(jnp.logical_and(before > 0, before < stops - 1))
        def _():
            got[c, h] = (total() + chain[c, h].astype(jnp.float32)).astype(jnp.bfloat16)

        @pl.when(before < stops - 1)
        def _():
            chain_copy(c, h).start()

        @pl.when(before == stops - 1)
        def _():
            both = total() + chain[c, h].astype(jnp.float32)
            gate = both[:, :WIDTH]
            hid[c, h, core] = (gate / (1.0 + jnp.exp(-gate)) * both[:, WIDTH:]).astype(jnp.bfloat16)
            back_copy(c, h).start()
            side_copy(c, h).start()

    def relay(c, h):
        before = done_before(h)

        @pl.when(before < stops - 1)
        def _():
            back_copy(c, h).wait_recv()

            @pl.when(before > 0)
            def _():
                back_copy(c, h).start()

            side_copy(c, h).start()

    def down(c, h):
        side_land(c, h).wait_recv()
        d_rows = d_buf[pl.ds(pl.multiple_of(c * WIDTH, WIDTH), WIDTH), :]
        for q in range(2):
            rows = slice(h * half + q * quarter, h * half + (q + 1) * quarter)
            acc[rows, :] += jnp.dot(hid[c, h, q], d_rows, preferred_element_type=jnp.float32)

    @pl.loop(0, chunks + 2 + (RS_LAG + AG_LAG) * (stops - 1))
    def _(t):
        rs_c = [t - 1 - RS_LAG * done_before(h) for h in range(2)]
        ag_c = [t - 1 - RS_LAG * (stops - 1) - AG_LAG * (stops - 1 - done_before(h)) for h in range(2)]

        for h in range(2):
            @pl.when(inside(rs_c[h]))
            def _(h=h):
                reduce(rs_c[h], h)

        for h in range(2):
            @pl.when(inside(ag_c[h]))
            def _(h=h):
                relay(ag_c[h], h)

        @pl.when(t < chunks)
        def _():
            multiply(t)

        @pl.when(t == 1 + RS_LAG * (stops - 1))
        def _():
            d_copy.wait()

        for h in range(2):
            @pl.when(inside(ag_c[h] - 1))
            def _(h=h):
                down(ag_c[h] - 1, h)

    out_ref[...] = acc[...].astype(out_ref.dtype)

    for j in range(tp_n - 1):
        x_copy(j).wait_send()

    @pl.loop(0, chunks)
    def _(c):
        for h in range(2):
            before = done_before(h)
            swap_copy(c, h).wait_send()
            side_copy(c, h).wait_send()

            @pl.when(before < stops - 1)
            def _(h=h):
                chain_copy(c, h).wait_send()

            @pl.when(before > 0)
            def _(h=h):
                back_copy(c, h).wait_send()


def ffn(x_sub, gate_weight, up_weight, down_weight, call):
    seq_n, tp_n = lax.axis_size("seq"), lax.axis_size("tp")
    sub, feats = x_sub.shape
    units = gate_weight.shape[1]
    cols = down_weight.shape[1]
    tokens = sub * tp_n
    quarter = tokens // 4
    n = units // WIDTH
    bf16 = jnp.bfloat16
    dma = pltpu.SemaphoreType.DMA
    vmem = pl.BlockSpec(memory_space=pltpu.VMEM)
    anywhere = pl.BlockSpec(memory_space=pl.ANY)
    return pl.pallas_call(
        functools.partial(ffn_kernel, seq_n, tp_n),
        out_shape=jax.ShapeDtypeStruct((tokens, cols), bf16),
        in_specs=[vmem, anywhere, anywhere, anywhere],
        out_specs=vmem,
        scratch_shapes=[
            pltpu.VMEM((tokens, feats), bf16),
            pltpu.VMEM((2, 2, feats, WIDTH), bf16),
            pltpu.VMEM((units, cols), bf16),
            pltpu.VMEM((n, 2, quarter, 2 * WIDTH), bf16),
            pltpu.VMEM((n, 2, quarter, 2 * WIDTH), bf16),
            pltpu.VMEM((n, 2, quarter, 2 * WIDTH), bf16),
            pltpu.VMEM((n, 2, quarter, 2 * WIDTH), bf16),
            pltpu.VMEM((n, 2, 2, quarter, WIDTH), bf16),
            pltpu.VMEM((tokens, cols), jnp.float32),
            dma((tp_n - 1,)), dma((tp_n - 1,)), dma(()), dma((2, 2)), dma(()),
            dma((2, n)), dma((2, n)), dma((2, n)), dma((2, n)), dma((2, n)), dma((2, n)), dma((2, n)), dma((2, n)),
        ],
        compiler_params=pltpu.CompilerParams(
            collective_id=call, has_side_effects=True, vmem_limit_bytes=63 * 1024 * 1024),
        cost_estimate=pl.CostEstimate(
            flops=6 * tokens * feats * units, bytes_accessed=6 * feats * units, transcendentals=0),
    )(x_sub, gate_weight, up_weight, down_weight)


def shards(tokens, conv_weight, norm_gain, gate_weight, up_weight, down_weight):
    tok_rows = tokens.shape[0]
    taps_count = conv_weight.shape[0]
    seq_count = lax.axis_size("seq")
    tp_count = lax.axis_size("tp")
    part_rows = tok_rows // tp_count
    edge_rows = from_behind(tokens[tok_rows - (taps_count - 1) :], "seq", 1)
    extended = jnp.concatenate([edge_rows, tokens], 0)
    extended = lax.dynamic_slice_in_dim(
        extended, lax.axis_index("tp") * part_rows, part_rows + taps_count - 1, 0).astype(jnp.float32)
    conv_out = jnp.zeros((part_rows, tokens.shape[1]), jnp.float32)
    for tap_index in range(taps_count):
        begin = taps_count - 1 - tap_index
        conv_out = conv_out + conv_weight[tap_index][None, :] * extended[begin : begin + part_rows]
    scale_rms = lax.rsqrt(jnp.mean(conv_out * conv_out, axis=-1, keepdims=True) + 1e-05)
    normed = (conv_out * scale_rms * norm_gain[None, :]).astype(jnp.bfloat16)
    x_sub = lax.all_to_all(normed, "seq", split_axis=1, concat_axis=0, tiled=True)
    blocks = max(1, x_sub.shape[0] * tp_count // BLOCK_TOKENS)
    rows = x_sub.shape[0] // blocks
    parts = [
        ffn(x_sub[b * rows : (b + 1) * rows], gate_weight, up_weight, down_weight, b).reshape(tp_count, rows, -1)
        for b in range(blocks)
    ]
    terms = parts[0] if blocks == 1 else jnp.concatenate(parts, 1)
    pieces = lax.all_to_all(terms, "tp", split_axis=0, concat_axis=0, tiled=True)
    summed = jnp.sum(pieces.astype(jnp.float32), 0).astype(jnp.bfloat16)
    summed = summed.reshape(seq_count, part_rows, -1)
    mixed_out = lax.all_to_all(summed, "seq", split_axis=0, concat_axis=2, tiled=True)
    return mixed_out.reshape(mixed_out.shape[1], mixed_out.shape[2])


def solution(mesh):
    in_specs = (P("seq", None), P(), P(), P("seq", "tp"), P("seq", "tp"), P("tp", "seq"))
    out_specs = P(("seq", "tp"), None)
    return jax.shard_map(shards, mesh=mesh, in_specs=in_specs, out_specs=out_specs, check_vma=False)
```

```python
import functools

import jax
import jax.numpy as jnp
from jax import lax
from jax.experimental import pallas as pl
from jax.experimental.pallas import tpu as pltpu
from jax.sharding import PartitionSpec as P

MESH = pl.DeviceIdType.MESH
WIDTH = 128
BLOCK_TOKENS = 1024
RS_LAG = 2
AG_LAG = 2


def from_behind(shard, axis, by):
    peers = lax.axis_size(axis)
    pairs = [(i, i + by) for i in range(peers) if 0 <= i + by < peers]
    return lax.ppermute(shard, axis, pairs)


def ffn_kernel(seq_n, tp_n, x_ref, gw_ref, uw_ref, dw_ref, out_ref, x_all, w_buf, d_buf, own, give, got, chain, hid, acc,
               x_snd, x_rcv, x_loc, w_sem, d_sem, p_snd, p_rcv, c_snd, c_rcv, h_snd, h_rcv, q_snd, q_rcv):
    stops = seq_n // 2
    seq_i = lax.axis_index("seq")
    tp_i = lax.axis_index("tp")
    pos = seq_i // 2
    core = seq_i % 2
    partner = (pos * 2 + 1 - core, tp_i)

    def at_stop(stop):
        return (stop * 2 + core, tp_i)

    sub = x_ref.shape[0]
    tokens = sub * tp_n
    half = tokens // 2
    quarter = half // 2
    chunks = gw_ref.shape[1] // WIDTH

    def w_copies(c):
        slot = c % 2
        cols = pl.ds(pl.multiple_of(c * WIDTH, WIDTH), WIDTH)
        return [
            pltpu.make_async_copy(gw_ref.at[:, cols], w_buf.at[slot, 0], w_sem.at[slot, 0]),
            pltpu.make_async_copy(uw_ref.at[:, cols], w_buf.at[slot, 1], w_sem.at[slot, 1]),
        ]

    for c in range(2):
        for cp in w_copies(c):
            cp.start()
    d_copy = pltpu.make_async_copy(dw_ref, d_buf, d_sem)
    d_copy.start()
    my_x = pl.ds(pl.multiple_of(tp_i * sub, sub), sub)
    x_own = pltpu.make_async_copy(x_ref, x_all.at[my_x], x_loc)
    x_own.start()

    barrier = pltpu.get_barrier_semaphore()
    greet = [partner, at_stop((pos + 1) % stops), at_stop((pos + stops - 1) % stops)]
    greet += [(seq_i, (tp_i + j) % tp_n) for j in range(1, tp_n)]
    for dev in greet:
        pl.semaphore_signal(barrier, inc=1, device_id=dev, device_id_type=MESH)
    pl.semaphore_wait(barrier, len(greet))

    def x_copy(j):
        return pltpu.make_async_remote_copy(
            src_ref=x_ref, dst_ref=x_all.at[my_x], send_sem=x_snd.at[j], recv_sem=x_rcv.at[j],
            device_id=(seq_i, (tp_i + j + 1) % tp_n), device_id_type=MESH)

    def x_land(j):
        origin = (tp_i + tp_n - j - 1) % tp_n
        rows = pl.ds(pl.multiple_of(origin * sub, sub), sub)
        return pltpu.make_async_remote_copy(
            src_ref=x_ref, dst_ref=x_all.at[rows], send_sem=x_snd.at[j], recv_sem=x_rcv.at[j],
            device_id=(seq_i, (tp_i + j + 1) % tp_n), device_id_type=MESH)

    for j in range(tp_n - 1):
        x_copy(j).start()
    acc[...] = jnp.zeros_like(acc)
    x_own.wait()
    for j in range(tp_n - 1):
        x_land(j).wait_recv()

    def swap_copy(c, h):
        return pltpu.make_async_remote_copy(
            src_ref=give.at[c, h], dst_ref=got.at[c, h], send_sem=p_snd.at[h, c], recv_sem=p_rcv.at[h, c],
            device_id=partner, device_id_type=MESH)

    def step_of(h):
        return -1 if h == 0 else 1

    def clamp(stop):
        return jnp.clip(stop, 0, stops - 1)

    def chain_copy(c, h):
        return pltpu.make_async_remote_copy(
            src_ref=got.at[c, h], dst_ref=chain.at[c, h], send_sem=c_snd.at[h, c], recv_sem=c_rcv.at[h, c],
            device_id=at_stop(pos + step_of(h)), device_id_type=MESH)

    def back_copy(c, h):
        return pltpu.make_async_remote_copy(
            src_ref=hid.at[c, h, core], dst_ref=hid.at[c, h, core], send_sem=h_snd.at[h, c], recv_sem=h_rcv.at[h, c],
            device_id=at_stop(pos - step_of(h)), device_id_type=MESH)

    def side_copy(c, h):
        return pltpu.make_async_remote_copy(
            src_ref=hid.at[c, h, core], dst_ref=hid.at[c, h, core], send_sem=q_snd.at[h, c], recv_sem=q_rcv.at[h, c],
            device_id=partner, device_id_type=MESH)

    def side_land(c, h):
        return pltpu.make_async_remote_copy(
            src_ref=hid.at[c, h, 1 - core], dst_ref=hid.at[c, h, 1 - core], send_sem=q_snd.at[h, c],
            recv_sem=q_rcv.at[h, c], device_id=partner, device_id_type=MESH)

    def done_before(h):
        return stops - 1 - pos if h == 0 else pos

    def inside(c):
        return jnp.logical_and(c >= 0, c < chunks)

    def multiply(c):
        slot = c % 2
        for cp in w_copies(c):
            cp.wait()
        for h in range(2):
            for mine in range(2):
                q = core if mine else 1 - core
                rows = x_all[pl.ds(pl.multiple_of(h * half + q * quarter, quarter), quarter), :]
                dest = own if mine else give
                for k in range(2):
                    part = jnp.dot(rows, w_buf[slot, k], preferred_element_type=jnp.float32)
                    dest[c, h, :, k * WIDTH : (k + 1) * WIDTH] = part.astype(jnp.bfloat16)
        for h in range(2):
            swap_copy(c, h).start()

        @pl.when(c + 2 < chunks)
        def _():
            for cp in w_copies(c + 2):
                cp.start()

    def reduce(c, h):
        swap_copy(c, h).wait_recv()
        before = done_before(h)
        total = lambda: own[c, h].astype(jnp.float32) + got[c, h].astype(jnp.float32)

        @pl.when(before == 0)
        def _():
            got[c, h] = total().astype(jnp.bfloat16)

        @pl.when(before > 0)
        def _():
            chain_copy(c, h).wait_recv()

        @pl.when(jnp.logical_and(before > 0, before < stops - 1))
        def _():
            got[c, h] = (total() + chain[c, h].astype(jnp.float32)).astype(jnp.bfloat16)

        @pl.when(before < stops - 1)
        def _():
            chain_copy(c, h).start()

        @pl.when(before == stops - 1)
        def _():
            both = total() + chain[c, h].astype(jnp.float32)
            gate = both[:, :WIDTH]
            hid[c, h, core] = (gate / (1.0 + jnp.exp(-gate)) * both[:, WIDTH:]).astype(jnp.bfloat16)
            back_copy(c, h).start()
            side_copy(c, h).start()

    def relay(c, h):
        before = done_before(h)

        @pl.when(before < stops - 1)
        def _():
            back_copy(c, h).wait_recv()

            @pl.when(before > 0)
            def _():
                back_copy(c, h).start()

            side_copy(c, h).start()

    def down(c, h):
        side_land(c, h).wait_recv()
        d_rows = d_buf[pl.ds(pl.multiple_of(c * WIDTH, WIDTH), WIDTH), :]
        for q in range(2):
            rows = slice(h * half + q * quarter, h * half + (q + 1) * quarter)
            acc[rows, :] += jnp.dot(hid[c, h, q], d_rows, preferred_element_type=jnp.float32)

    @pl.loop(0, chunks + 2 + (RS_LAG + AG_LAG) * (stops - 1))
    def _(t):
        rs_c = [t - 1 - RS_LAG * done_before(h) for h in range(2)]
        ag_c = [t - 1 - RS_LAG * (stops - 1) - AG_LAG * (stops - 1 - done_before(h)) for h in range(2)]

        for h in range(2):
            @pl.when(inside(rs_c[h]))
            def _(h=h):
                reduce(rs_c[h], h)

        for h in range(2):
            @pl.when(inside(ag_c[h]))
            def _(h=h):
                relay(ag_c[h], h)

        @pl.when(t < chunks)
        def _():
            multiply(t)

        @pl.when(t == 1 + RS_LAG * (stops - 1))
        def _():
            d_copy.wait()

        for h in range(2):
            @pl.when(inside(ag_c[h] - 1))
            def _(h=h):
                down(ag_c[h] - 1, h)

    out_ref[...] = acc[...].astype(out_ref.dtype)

    for j in range(tp_n - 1):
        x_copy(j).wait_send()

    @pl.loop(0, chunks)
    def _(c):
        for h in range(2):
            before = done_before(h)
            swap_copy(c, h).wait_send()
            side_copy(c, h).wait_send()

            @pl.when(before < stops - 1)
            def _(h=h):
                chain_copy(c, h).wait_send()

            @pl.when(before > 0)
            def _(h=h):
                back_copy(c, h).wait_send()


def ffn(x_sub, gate_weight, up_weight, down_weight, call):
    seq_n, tp_n = lax.axis_size("seq"), lax.axis_size("tp")
    sub, feats = x_sub.shape
    units = gate_weight.shape[1]
    cols = down_weight.shape[1]
    tokens = sub * tp_n
    quarter = tokens // 4
    n = units // WIDTH
    bf16 = jnp.bfloat16
    dma = pltpu.SemaphoreType.DMA
    vmem = pl.BlockSpec(memory_space=pltpu.VMEM)
    anywhere = pl.BlockSpec(memory_space=pl.ANY)
    return pl.pallas_call(
        functools.partial(ffn_kernel, seq_n, tp_n),
        out_shape=jax.ShapeDtypeStruct((tokens, cols), bf16),
        in_specs=[vmem, anywhere, anywhere, anywhere],
        out_specs=vmem,
        scratch_shapes=[
            pltpu.VMEM((tokens, feats), bf16),
            pltpu.VMEM((2, 2, feats, WIDTH), bf16),
            pltpu.VMEM((units, cols), bf16),
            pltpu.VMEM((n, 2, quarter, 2 * WIDTH), bf16),
            pltpu.VMEM((n, 2, quarter, 2 * WIDTH), bf16),
            pltpu.VMEM((n, 2, quarter, 2 * WIDTH), bf16),
            pltpu.VMEM((n, 2, quarter, 2 * WIDTH), bf16),
            pltpu.VMEM((n, 2, 2, quarter, WIDTH), bf16),
            pltpu.VMEM((tokens, cols), jnp.float32),
            dma((tp_n - 1,)), dma((tp_n - 1,)), dma(()), dma((2, 2)), dma(()),
            dma((2, n)), dma((2, n)), dma((2, n)), dma((2, n)), dma((2, n)), dma((2, n)), dma((2, n)), dma((2, n)),
        ],
        compiler_params=pltpu.CompilerParams(
            collective_id=call, has_side_effects=True, vmem_limit_bytes=63 * 1024 * 1024),
        cost_estimate=pl.CostEstimate(
            flops=6 * tokens * feats * units, bytes_accessed=6 * feats * units, transcendentals=0),
    )(x_sub, gate_weight, up_weight, down_weight)


def shards(tokens, conv_weight, norm_gain, gate_weight, up_weight, down_weight):
    tok_rows = tokens.shape[0]
    taps_count = conv_weight.shape[0]
    seq_count = lax.axis_size("seq")
    tp_count = lax.axis_size("tp")
    part_rows = tok_rows // tp_count
    edge_rows = from_behind(tokens[tok_rows - (taps_count - 1) :], "seq", 1)
    extended = jnp.concatenate([edge_rows, tokens], 0)
    extended = lax.dynamic_slice_in_dim(
        extended, lax.axis_index("tp") * part_rows, part_rows + taps_count - 1, 0).astype(jnp.float32)
    conv_out = jnp.zeros((part_rows, tokens.shape[1]), jnp.float32)
    for tap_index in range(taps_count):
        begin = taps_count - 1 - tap_index
        conv_out = conv_out + conv_weight[tap_index][None, :] * extended[begin : begin + part_rows]
    scale_rms = lax.rsqrt(jnp.mean(conv_out * conv_out, axis=-1, keepdims=True) + 1e-05)
    normed = (conv_out * scale_rms * norm_gain[None, :]).astype(jnp.bfloat16)
    x_sub = lax.all_to_all(normed, "seq", split_axis=1, concat_axis=0, tiled=True)
    blocks = max(1, x_sub.shape[0] * tp_count // BLOCK_TOKENS)
    rows = x_sub.shape[0] // blocks
    parts = [
        ffn(x_sub[b * rows : (b + 1) * rows], gate_weight, up_weight, down_weight, b).reshape(tp_count, rows, -1)
        for b in range(blocks)
    ]
    terms = parts[0] if blocks == 1 else jnp.concatenate(parts, 1)
    pieces = lax.all_to_all(terms, "tp", split_axis=0, concat_axis=0, tiled=True)
    summed = jnp.sum(pieces.astype(jnp.float32), 0).astype(jnp.bfloat16)
    summed = summed.reshape(seq_count, part_rows, -1)
    mixed_out = lax.all_to_all(summed, "seq", split_axis=0, concat_axis=2, tiled=True)
    return mixed_out.reshape(mixed_out.shape[1], mixed_out.shape[2])


def solution(mesh):
    in_specs = (P("seq", None), P(), P(), P("seq", "tp"), P("seq", "tp"), P("tp", "seq"))
    out_specs = P(("seq", "tp"), None)
    return jax.shard_map(shards, mesh=mesh, in_specs=in_specs, out_specs=out_specs, check_vma=False)
```
